16 devices in a mesh: replica: 2 (over y, z), dp: 8 (over x, core).
Axes of the slice: x: 4, y: 2, z: 1, core: 2. Of those that a mesh axis runs over, the one named last changes fastest.
The devices are a block of a 4x4x8 slice.
Arguments:
- x: bfloat16 [1024, 2048], P(('replica', 'dp')), parts along dimension 0
- lengths: int32 [1024], P(('replica', 'dp')), parts along dimension 0
- cache: bfloat16 [2, 1024, 256, 576], P(None, ('replica', 'dp')), parts along dimension 1
- attn_gain: float32 [2, 2048], replicated
- ffn_gain: float32 [2, 2048], replicated
- w_query: bfloat16 [2, 2048, 9216], replicated
- w_attn_out: bfloat16 [2, 8192, 2048], replicated
- w_up: bfloat16 [2, 2048, 10944], P(None, None, 'dp')
- w_gate: bfloat16 [2, 2048, 10944], P(None, None, 'dp')
- w_down: bfloat16 [2, 10944, 2048], P(None, 'dp')
Outputs:
- output: bfloat16 [1024, 2048], P(('replica', 'dp')), parts along dimension 0
There are 2 independent parts. The reference program is written for one: setup_inputs(seed, part) draws one part's arguments, and reference() takes and returns one part's arrays. A program takes and returns all parts, laid end to end along the dimension named above; an argument that names none is the same for every part.
All inputs are finite; a program needn't handle non-finite values.
Results may differ from the reference program's by a relative error of at most 0.02.
Values are sent between devices in bfloat16 or wider.
A program may use at most 768 MiB of HBM per device.

```python
import jax
import jax.numpy as jnp
from jax import lax

B_DEV = 64
GROUP_SIZE = 8
SEQ_LEN = 256
D_MODEL = 2048
FF_DIM = 10944
HEADS = 16
LATENT = 512
ROPE = 64
LAYERS = 2

NORM_EPS = 1e-6
BATCH = B_DEV * GROUP_SIZE
KV_DIM = LATENT + ROPE
SCORE_SCALE = (3 * ROPE) ** -0.5
LEN_FLOOR = max(1, SEQ_LEN // 16)
CAP_FLOOR = max(LEN_FLOOR, SEQ_LEN // 4)


def draw_lengths(key):
    cap_key, len_key, pick_key = jax.random.split(key, 3)
    caps = jax.random.randint(cap_key, (GROUP_SIZE,), CAP_FLOOR, SEQ_LEN + 1)
    full_dev = jax.random.randint(pick_key, (), 0, GROUP_SIZE)
    caps = jnp.where(jnp.arange(GROUP_SIZE) == full_dev, SEQ_LEN, caps)
    drawn = jax.random.randint(len_key, (GROUP_SIZE, B_DEV), LEN_FLOOR, caps[:, None] + 1)
    drawn = jnp.concatenate([drawn[:, 1:], caps[:, None]], axis=1)
    return jnp.sort(drawn, axis=1).reshape(BATCH).astype(jnp.int32)


def setup_inputs(seed: int = 0, part: int = 0) -> dict:
    part_key = jax.random.fold_in(jax.random.key(seed), part)
    x_key, len_key, cache_key = jax.random.split(part_key, 3)
    shared_keys = jax.random.split(jax.random.key(seed + 1), 7)
    wo_scale = (HEADS * LATENT) ** -0.5 * max(1.0, (SEQ_LEN / 64) ** 0.5)
    return {
        'x': jax.random.normal(x_key, (BATCH, D_MODEL), jnp.float32).astype(jnp.bfloat16),
        'lengths': draw_lengths(len_key),
        'cache': jax.random.normal(cache_key, (LAYERS, BATCH, SEQ_LEN, KV_DIM), jnp.float32).astype(jnp.bfloat16),
        'attn_gain': 0.5 + jax.random.uniform(shared_keys[0], (LAYERS, D_MODEL), jnp.float32),
        'ffn_gain': 0.5 + jax.random.uniform(shared_keys[1], (LAYERS, D_MODEL), jnp.float32),
        'w_query': (jax.random.normal(shared_keys[2], (LAYERS, D_MODEL, HEADS * KV_DIM), jnp.float32) * D_MODEL ** -0.5).astype(jnp.bfloat16),
        'w_attn_out': (jax.random.normal(shared_keys[3], (LAYERS, HEADS * LATENT, D_MODEL), jnp.float32) * wo_scale).astype(jnp.bfloat16),
        'w_up': (jax.random.normal(shared_keys[4], (LAYERS, D_MODEL, FF_DIM), jnp.float32) * D_MODEL ** -0.5).astype(jnp.bfloat16),
        'w_gate': (jax.random.normal(shared_keys[5], (LAYERS, D_MODEL, FF_DIM), jnp.float32) * D_MODEL ** -0.5).astype(jnp.bfloat16),
        'w_down': (jax.random.normal(shared_keys[6], (LAYERS, FF_DIM, D_MODEL), jnp.float32) * 2.0 * FF_DIM ** -0.5).astype(jnp.bfloat16),
    }


def rms_norm(rows, gain):
    rows_f = rows.astype(jnp.float32)
    mean_sq = jnp.mean(rows_f * rows_f, axis=-1, keepdims=True)
    return (rows_f * lax.rsqrt(mean_sq + NORM_EPS) * gain).astype(jnp.bfloat16)


def attention_layer(x_all, lengths, cache_l, gain, wq_l, wo_l):
    x_blocks = x_all.reshape(GROUP_SIZE, B_DEV, D_MODEL)
    len_blocks = lengths.reshape(GROUP_SIZE, B_DEV)
    cache_blocks = cache_l.reshape(GROUP_SIZE, B_DEV, SEQ_LEN, KV_DIM)
    positions = jnp.arange(SEQ_LEN)[None, None, :]

    def one_block(block):
        x_rows, len_rows, cache_rows = block
        normed = rms_norm(x_rows, gain)
        query = jnp.dot(normed, wq_l, preferred_element_type=jnp.float32).astype(jnp.bfloat16)
        query = query.reshape(B_DEV, HEADS, KV_DIM).astype(jnp.float32)
        cache_f = cache_rows.astype(jnp.float32)
        scores = jnp.einsum('bhc,btc->bht', query, cache_f) * SCORE_SCALE
        scores = jnp.where(positions < len_rows[:, None, None], scores, -jnp.inf)
        attn_probs = jax.nn.softmax(scores, axis=-1).astype(jnp.bfloat16).astype(jnp.float32)
        mixed = jnp.einsum('bht,btc->bhc', attn_probs, cache_f[:, :, :LATENT]).astype(jnp.bfloat16)
        attn_out = jnp.dot(mixed.reshape(B_DEV, HEADS * LATENT), wo_l, preferred_element_type=jnp.float32)
        return (x_rows.astype(jnp.float32) + attn_out).astype(jnp.bfloat16)

    return lax.map(one_block, (x_blocks, len_blocks, cache_blocks)).reshape(BATCH, D_MODEL)


def ffn_layer(x_all, gain, wu_l, wg_l, wd_l):
    normed = rms_norm(x_all, gain)
    gate_pre = jnp.dot(normed, wg_l, preferred_element_type=jnp.float32)
    up_pre = jnp.dot(normed, wu_l, preferred_element_type=jnp.float32)
    hidden = (jax.nn.silu(gate_pre) * up_pre).astype(jnp.bfloat16)
    ffn_out = jnp.dot(hidden, wd_l, preferred_element_type=jnp.float32)
    return (x_all.astype(jnp.float32) + ffn_out).astype(jnp.bfloat16)


def reference(x, lengths, cache, attn_gain, ffn_gain, w_query, w_attn_out, w_up, w_gate, w_down):
    def layer_step(x_cur, params):
        cache_l, gain_a, gain_f, wq_l, wo_l, wu_l, wg_l, wd_l = params
        x_cur = attention_layer(x_cur, lengths, cache_l, gain_a, wq_l, wo_l)
        x_cur = ffn_layer(x_cur, gain_f, wu_l, wg_l, wd_l)
        return x_cur, None

    x_final, _ = lax.scan(layer_step, x, (cache, attn_gain, ffn_gain, w_query, w_attn_out, w_up, w_gate, w_down))
    return x_final
```

```python
import functools

import jax
import jax.numpy as jnp
from jax import lax
from jax.experimental import pallas as pl
from jax.experimental.pallas import tpu as pltpu
from jax.sharding import PartitionSpec as P

NORM_EPS = 1e-6
MESH = pl.DeviceIdType.MESH
NT = (((1,), (1,)), ((), ()))


def rms_norm(rows, gain):
    rows_f = rows.astype(jnp.float32)
    mean_sq = jnp.mean(rows_f * rows_f, axis=-1, keepdims=True)
    return (rows_f * lax.rsqrt(mean_sq + NORM_EPS) * gain).astype(jnp.bfloat16)


GROUP = 4
DEPTH = 4


def attention_kernel(layer, latent, scale, len_ref, q_ref, cache_ref, o_ref, buf, sem):
    rows, heads, kv = q_ref.shape
    seq = cache_ref.shape[3]
    half = seq // 2
    groups = rows // GROUP

    def is_short(g):
        return len_ref[g * GROUP + GROUP - 1] <= half

    def copy(g, width):
        slot = lax.rem(g, DEPTH)
        return pltpu.make_async_copy(
            cache_ref.at[layer, pl.ds(g * GROUP, GROUP), :, pl.ds(0, width)],
            buf.at[slot, :, :, pl.ds(0, width)],
            sem.at[slot],
        )

    def start(g):
        short = is_short(g)

        @pl.when(short)
        def _():
            copy(g, half).start()

        @pl.when(jnp.logical_not(short))
        def _():
            copy(g, seq).start()

    def compute(g, width):
        slot = lax.rem(g, DEPTH)
        copy(g, width).wait()
        for i in range(GROUP):
            b = g * GROUP + i
            keys = buf[slot, i, :, pl.ds(0, width)]
            s = jnp.dot(q_ref[b], keys, preferred_element_type=jnp.float32) * scale
            pos = lax.broadcasted_iota(jnp.int32, (heads, width), 1)
            s = jnp.where(pos < len_ref[b], s, -jnp.inf)
            e = jnp.exp(s - jnp.max(s, axis=1, keepdims=True))
            p = (e / jnp.sum(e, axis=1, keepdims=True)).astype(jnp.bfloat16)
            vals = buf[slot, i, pl.ds(0, latent), pl.ds(0, width)]
            o = lax.dot_general(p, vals, NT, preferred_element_type=jnp.float32)
            o_ref[b] = o.astype(jnp.bfloat16)

    for g in range(DEPTH - 1):
        start(g)

    def body(g, carry):
        @pl.when(g + DEPTH - 1 < groups)
        def _():
            start(g + DEPTH - 1)

        short = is_short(g)

        @pl.when(short)
        def _():
            compute(g, half)

        @pl.when(jnp.logical_not(short))
        def _():
            compute(g, seq)

        return carry

    lax.fori_loop(0, groups, body, 0)


def attention(layer, latent, q, cache_t, lengths):
    rows, heads, kv = q.shape
    seq = cache_t.shape[3]
    scale = (3 * (kv - latent)) ** -0.5
    return pl.pallas_call(
        functools.partial(attention_kernel, layer, latent, scale),
        out_shape=jax.ShapeDtypeStruct((rows, heads, latent), jnp.bfloat16),
        grid_spec=pltpu.PrefetchScalarGridSpec(
            num_scalar_prefetch=1,
            grid=(),
            in_specs=[
                pl.BlockSpec(memory_space=pltpu.VMEM),
                pl.BlockSpec(memory_space=pl.ANY),
            ],
            out_specs=pl.BlockSpec(memory_space=pltpu.VMEM),
            scratch_shapes=[
                pltpu.VMEM((DEPTH, GROUP, kv, seq), jnp.bfloat16),
                pltpu.SemaphoreType.DMA((DEPTH,)),
            ],
        ),
        compiler_params=pltpu.CompilerParams(vmem_limit_bytes=24 * 2**20),
        name=f"attention_{layer}",
    )(lengths, q, cache_t)


OWN, RIGHT, LEFT, OPP = 0, 1, 2, 3


def ffn_kernel(layer, n_dp, x_ref, g_ref, wu_hbm, wg_hbm, wd_hbm, out_ref,
               wu, wg, wd, g_all, act, part, sib_in, mid_l, mid_r, fin_l, fin_r,
               w_sem, send_sem, recv_sem):
    me = lax.axis_index("dp")
    chips = n_dp // 2
    chip, core = me // 2, lax.rem(me, 2)
    sib = chip * 2 + (1 - core)
    right = lax.rem(chip + 1, chips) * 2 + core
    left = lax.rem(chip + chips - 1, chips) * 2 + core
    rows, d_model = x_ref.shape
    hidden = wu_hbm.shape[1]
    hidden_pad = wu.shape[0]
    half = rows // 2

    w_copies = [
        pltpu.make_async_copy(src.at[layer], dst.at[pl.ds(0, hidden)], w_sem.at[i])
        for i, (src, dst) in enumerate(((wg_hbm, wg), (wu_hbm, wu), (wd_hbm, wd)))
    ]
    for c in w_copies:
        c.start()

    barrier = pltpu.get_barrier_semaphore()
    for peer in (sib, left, right):
        pl.semaphore_signal(barrier, inc=1, device_id={"dp": peer}, device_id_type=MESH)
    pl.semaphore_wait(barrier, 3)

    copies = []

    def send(src, dst, peer):
        k = len(copies)
        c = pltpu.make_async_remote_copy(
            src_ref=src, dst_ref=dst, send_sem=send_sem.at[k], recv_sem=recv_sem.at[k],
            device_id={"dp": peer}, device_id_type=MESH)
        copies.append(c)
        c.start()
        return c

    def at(slot, c, lo, n):
        return pl.ds(slot * 2 * rows + c * rows + lo, n)

    ag_sib = send(g_ref, g_all.at[at(OWN, core, 0, rows)], sib)
    ag_la = send(g_ref.at[pl.ds(0, half)], g_all.at[at(LEFT, core, 0, half)], right)
    ag_rb = send(g_ref.at[pl.ds(half, half)], g_all.at[at(RIGHT, core, half, half)], left)
    ag_lb = send(g_ref.at[pl.ds(half, half)], g_all.at[at(LEFT, core, half, half)], right)
    ag_ra = send(g_ref.at[pl.ds(0, half)], g_all.at[at(RIGHT, core, 0, half)], left)
    g_all[at(OWN, core, 0, rows), :] = g_ref[...]

    for w in (wu, wg, wd):
        w[pl.ds(hidden, hidden_pad - hidden), :] = jnp.zeros((hidden_pad - hidden, d_model), jnp.bfloat16)

    tile = 512

    def gate_up(lo, m):
        def body(j, carry):
            cols = pl.ds(pl.multiple_of(j * tile, tile), tile)
            g = g_all[pl.ds(lo, m), :]
            gate = lax.dot_general(g, wg[cols, :], NT, preferred_element_type=jnp.float32)
            up = lax.dot_general(g, wu[cols, :], NT, preferred_element_type=jnp.float32)
            act[pl.ds(0, m), cols] = (jax.nn.silu(gate) * up).astype(jnp.bfloat16)
            return carry

        lax.fori_loop(0, hidden_pad // tile, body, 0)

    def down(lo, m):
        def body(j, carry):
            cols = pl.ds(pl.multiple_of(j * tile, tile), tile)
            part[pl.ds(lo, m), cols] = jnp.dot(
                act[pl.ds(0, m), :], wd[:, cols], preferred_element_type=jnp.float32)
            return carry

        lax.fori_loop(0, d_model // tile, body, 0)

    def to_sib(slot):
        return send(part.at[at(slot, 1 - core, 0, rows)], sib_in.at[slot], sib)

    def add_sib(slot):
        r = at(slot, core, 0, rows)
        part[r, :] = part[r, :] + sib_in[slot]

    w_copies[0].wait()
    w_copies[1].wait()
    ag_sib.wait_recv()
    gate_up(0, 2 * rows)
    w_copies[2].wait()
    down(0, 2 * rows)
    rs_own = to_sib(OWN)

    ag_la.wait_recv()
    fwd_r = send(g_all.at[at(LEFT, core, 0, half)], g_all.at[at(OPP, core, 0, half)], right)
    d_la = send(g_all.at[at(LEFT, core, 0, half)], g_all.at[at(LEFT, core, 0, half)], sib)
    ag_rb.wait_recv()
    fwd_l = send(g_all.at[at(RIGHT, core, half, half)], g_all.at[at(OPP, core, half, half)], left)
    d_rb = send(g_all.at[at(RIGHT, core, half, half)], g_all.at[at(RIGHT, core, half, half)], sib)
    ag_lb.wait_recv()
    d_lb = send(g_all.at[at(LEFT, core, half, half)], g_all.at[at(LEFT, core, half, half)], sib)
    ag_ra.wait_recv()
    d_ra = send(g_all.at[at(RIGHT, core, 0, half)], g_all.at[at(RIGHT, core, 0, half)], sib)
    for c in (d_la, d_rb, d_lb, d_ra):
        c.wait_recv()

    gate_up(2 * rows, 4 * rows)
    fwd_r.wait_recv()
    d_oa = send(g_all.at[at(OPP, core, 0, half)], g_all.at[at(OPP, core, 0, half)], sib)
    fwd_l.wait_recv()
    d_ob = send(g_all.at[at(OPP, core, half, half)], g_all.at[at(OPP, core, half, half)], sib)
    down(2 * rows, 4 * rows)
    rs_r = to_sib(RIGHT)
    rs_l = to_sib(LEFT)

    d_oa.wait_recv()
    d_ob.wait_recv()
    gate_up(6 * rows, 2 * rows)

    rs_r.wait_recv()
    add_sib(RIGHT)
    direct_r = send(part.at[at(RIGHT, core, half, half)], fin_l.at[pl.ds(half, half)], right)
    rs_l.wait_recv()
    add_sib(LEFT)
    direct_l = send(part.at[at(LEFT, core, 0, half)], fin_r.at[pl.ds(0, half)], left)

    down(6 * rows, 2 * rows)
    rs_o = to_sib(OPP)
    rs_o.wait_recv()
    add_sib(OPP)
    opp_r = send(part.at[at(OPP, core, 0, half)], mid_l, right)
    opp_l = send(part.at[at(OPP, core, half, half)], mid_r, left)

    opp_r.wait_recv()
    r = at(RIGHT, core, 0, half)
    part[r, :] = part[r, :] + mid_l[...]
    merged_r = send(part.at[r], fin_l.at[pl.ds(0, half)], right)
    opp_l.wait_recv()
    r = at(LEFT, core, half, half)
    part[r, :] = part[r, :] + mid_r[...]
    merged_l = send(part.at[r], fin_r.at[pl.ds(half, half)], left)

    rs_own.wait_recv()
    total = part[at(OWN, core, 0, rows), :] + sib_in[OWN]
    for c in (direct_r, direct_l, merged_r, merged_l):
        c.wait_recv()
    total = total + fin_l[...] + fin_r[...]
    out_ref[...] = (x_ref[...].astype(jnp.float32) + total).astype(jnp.bfloat16)
    for c in copies:
        c.wait_send()


N_COPIES = 23


def ffn(layer, n_dp, x_rows, normed, wu_t, wg_t, wd):
    rows, d_model = x_rows.shape
    hidden = wd.shape[1]
    hidden_pad = pl.cdiv(hidden, 512) * 512
    all_rows = rows * n_dp
    vmem = pl.BlockSpec(memory_space=pltpu.VMEM)
    hbm = pl.BlockSpec(memory_space=pl.ANY)
    return pl.pallas_call(
        functools.partial(ffn_kernel, layer, n_dp),
        out_shape=jax.ShapeDtypeStruct((rows, d_model), jnp.bfloat16),
        in_specs=[vmem, vmem, hbm, hbm, hbm],
        out_specs=vmem,
        scratch_shapes=[
            pltpu.VMEM((hidden_pad, d_model), jnp.bfloat16),
            pltpu.VMEM((hidden_pad, d_model), jnp.bfloat16),
            pltpu.VMEM((hidden_pad, d_model), jnp.bfloat16),
            pltpu.VMEM((all_rows, d_model), jnp.bfloat16),
            pltpu.VMEM((4 * rows, hidden_pad), jnp.bfloat16),
            pltpu.VMEM((all_rows, d_model), jnp.float32),
            pltpu.VMEM((4, rows, d_model), jnp.float32),
            pltpu.VMEM((rows // 2, d_model), jnp.float32),
            pltpu.VMEM((rows // 2, d_model), jnp.float32),
            pltpu.VMEM((rows, d_model), jnp.float32),
            pltpu.VMEM((rows, d_model), jnp.float32),
            pltpu.SemaphoreType.DMA((3,)),
            pltpu.SemaphoreType.DMA((N_COPIES,)),
            pltpu.SemaphoreType.DMA((N_COPIES,)),
        ],
        compiler_params=pltpu.CompilerParams(
            collective_id=layer, has_side_effects=True, vmem_limit_bytes=48 * 2**20),
        name=f"ffn_{layer}",
    )(x_rows, normed, wu_t, wg_t, wd)


def solution(mesh):
    row_axes = ('replica', 'dp')
    n_dp = mesh.shape['dp']

    def local_step(x_rows, lengths, cache, attn_gain, ffn_gain, w_query, w_attn_out, w_up, w_gate, w_down):
        cache_t = jnp.swapaxes(cache, 2, 3)
        wu_t = jnp.swapaxes(w_up, 1, 2)
        wg_t = jnp.swapaxes(w_gate, 1, 2)
        layers, rows, seq, kv_dim = cache.shape
        heads = w_query.shape[2] // kv_dim
        latent = w_attn_out.shape[1] // heads
        for l in range(layers):
            h = rms_norm(x_rows, attn_gain[l])
            q = jnp.dot(h, w_query[l], preferred_element_type=jnp.float32).astype(jnp.bfloat16)
            o = attention(l, latent, q.reshape(rows, heads, kv_dim), cache_t, lengths)
            proj = jnp.dot(o.reshape(rows, heads * latent), w_attn_out[l], preferred_element_type=jnp.float32)
            x_rows = (x_rows.astype(jnp.float32) + proj).astype(jnp.bfloat16)
            g = rms_norm(x_rows, ffn_gain[l])
            x_rows = ffn(l, n_dp, x_rows, g, wu_t, wg_t, w_down)
        return x_rows

    return jax.shard_map(
        local_step,
        mesh=mesh,
        in_specs=(P(row_axes, None), P(row_axes), P(None, row_axes, None, None), P(), P(), P(), P(),
                  P(None, None, 'dp'), P(None, None, 'dp'), P(None, 'dp', None)),
        out_specs=P(row_axes, None),
        check_vma=False,
    )
```

```python
import functools

import jax
import jax.numpy as jnp
from jax import lax
from jax.experimental import pallas as pl
from jax.experimental.pallas import tpu as pltpu
from jax.sharding import PartitionSpec as P

NORM_EPS = 1e-6
MESH = pl.DeviceIdType.MESH
NT = (((1,), (1,)), ((), ()))


def rms_norm(rows, gain):
    rows_f = rows.astype(jnp.float32)
    mean_sq = jnp.mean(rows_f * rows_f, axis=-1, keepdims=True)
    return (rows_f * lax.rsqrt(mean_sq + NORM_EPS) * gain).astype(jnp.bfloat16)


GROUP = 8
DEPTH = 3


def attention_kernel(layer, latent, scale, len_ref, q_ref, cache_ref, o_ref, buf, sem):
    rows, heads, kv = q_ref.shape
    seq = cache_ref.shape[3]
    half = seq // 2
    groups = rows // GROUP

    def is_short(g):
        return len_ref[g * GROUP + GROUP - 1] <= half

    def copy(g, width):
        slot = lax.rem(g, DEPTH)
        return pltpu.make_async_copy(
            cache_ref.at[layer, pl.ds(g * GROUP, GROUP), :, pl.ds(0, width)],
            buf.at[slot, :, :, pl.ds(0, width)],
            sem.at[slot],
        )

    def start(g):
        short = is_short(g)

        @pl.when(short)
        def _():
            copy(g, half).start()

        @pl.when(jnp.logical_not(short))
        def _():
            copy(g, seq).start()

    def compute(g, width):
        slot = lax.rem(g, DEPTH)
        copy(g, width).wait()
        bs = [g * GROUP + i for i in range(GROUP)]
        s = [jnp.dot(q_ref[b], buf[slot, i, :, pl.ds(0, width)], preferred_element_type=jnp.float32)
             for i, b in enumerate(bs)]
        pos = lax.broadcasted_iota(jnp.int32, (heads, width), 1)
        s = [jnp.where(pos < len_ref[b], x * scale, -jnp.inf) for x, b in zip(s, bs)]
        e = [jnp.exp(x - jnp.max(x, axis=1, keepdims=True)) for x in s]
        p = [(x / jnp.sum(x, axis=1, keepdims=True)).astype(jnp.bfloat16) for x in e]
        o = [lax.dot_general(x, buf[slot, i, pl.ds(0, latent), pl.ds(0, width)], NT,
                             preferred_element_type=jnp.float32) for i, x in enumerate(p)]
        for x, b in zip(o, bs):
            o_ref[b] = x.astype(jnp.bfloat16)

    for g in range(DEPTH - 1):
        start(g)

    def body(g, carry):
        @pl.when(g + DEPTH - 1 < groups)
        def _():
            start(g + DEPTH - 1)

        short = is_short(g)

        @pl.when(short)
        def _():
            compute(g, half)

        @pl.when(jnp.logical_not(short))
        def _():
            compute(g, seq)

        return carry

    lax.fori_loop(0, groups, body, 0)


def attention(layer, latent, q, cache_t, lengths):
    rows, heads, kv = q.shape
    seq = cache_t.shape[3]
    scale = (3 * (kv - latent)) ** -0.5
    return pl.pallas_call(
        functools.partial(attention_kernel, layer, latent, scale),
        out_shape=jax.ShapeDtypeStruct((rows, heads, latent), jnp.bfloat16),
        grid_spec=pltpu.PrefetchScalarGridSpec(
            num_scalar_prefetch=1,
            grid=(),
            in_specs=[
                pl.BlockSpec(memory_space=pltpu.VMEM),
                pl.BlockSpec(memory_space=pl.ANY),
            ],
            out_specs=pl.BlockSpec(memory_space=pltpu.VMEM),
            scratch_shapes=[
                pltpu.VMEM((DEPTH, GROUP, kv, seq), jnp.bfloat16),
                pltpu.SemaphoreType.DMA((DEPTH,)),
            ],
        ),
        compiler_params=pltpu.CompilerParams(vmem_limit_bytes=24 * 2**20),
        name=f"attention_{layer}",
    )(lengths, q, cache_t)


NEAR, FAR, NEXT, OWN = 0, 1, 2, 3
TILE = 512
HID_TILE = 512
N_COPIES = 31


def dense_kernel(ffn_layer, q_layer, n_dp, *refs):
    refs = list(refs)

    def take(n):
        out = refs[:n]
        del refs[:n]
        return out

    (x_ref,) = take(1)
    if ffn_layer is not None:
        o_ref, fgain_ref, wo_hbm, wu_hbm, wg_hbm, wd_hbm = take(6)
    if q_layer is not None:
        again_ref, wq_hbm = take(2)
    if ffn_layer is not None:
        (xout_ref,) = take(1)
    if q_layer is not None:
        (q_ref,) = take(1)
    (wt,) = take(1)
    if ffn_layer is not None:
        (o_all, proj, proj_in, x_mid, wu, wg, wd, g_all, act, part, sib_in, mid_l, mid_r, fin_l, fin_r) = take(15)
    if q_layer is not None:
        h_all, q_all, q_in = take(3)
    wt_sem, w_sem, send_sem, recv_sem = refs

    me = lax.axis_index("dp")
    chips = n_dp // 2
    chip, core = me // 2, lax.rem(me, 2)
    other = 1 - core
    sib = chip * 2 + other
    right = lax.rem(chip + 1, chips) * 2 + core
    left = lax.rem(chip + chips - 1, chips) * 2 + core
    rows, d_model = x_ref.shape
    half, quarter = rows // 2, rows // 4
    depth = wt.shape[1]

    def q_copy(t):
        cols = q_ref.shape[1] // 2
        lo = pl.multiple_of(core * cols + t * TILE, TILE // 4)
        return pltpu.make_async_copy(wq_hbm.at[q_layer, :, pl.ds(lo, TILE)], wt.at[t], wt_sem.at[t])

    if q_layer is not None:
        n_q = q_ref.shape[1] // 2 // TILE

    if ffn_layer is not None:
        k_steps = o_ref.shape[1] // depth
        n_o = d_model // 2 // TILE

        def o_copy(t):
            n, k = t // k_steps, lax.rem(t, k_steps)
            lo = pl.multiple_of(core * (d_model // 2) + n * TILE, TILE)
            return pltpu.make_async_copy(
                wo_hbm.at[ffn_layer, pl.ds(pl.multiple_of(k * depth, depth), depth), pl.ds(lo, TILE)],
                wt.at[t], wt_sem.at[t])

        for t in range(n_o * k_steps):
            o_copy(t).start()
    else:
        for t in range(n_q):
            q_copy(t).start()

    barrier = pltpu.get_barrier_semaphore()
    peers = (sib,) if ffn_layer is None else (sib, left, right)
    for peer in peers:
        pl.semaphore_signal(barrier, inc=1, device_id={"dp": peer}, device_id_type=MESH)

    copies = []

    def send(src, dst, peer):
        k = len(copies)
        c = pltpu.make_async_remote_copy(
            src_ref=src, dst_ref=dst, send_sem=send_sem.at[k], recv_sem=recv_sem.at[k],
            device_id={"dp": peer}, device_id_type=MESH)
        copies.append(c)
        c.start()
        return c

    mine, theirs = pl.ds(core * rows, rows), pl.ds(other * rows, rows)

    def norm(x_f, gain):
        mean_sq = jnp.mean(x_f * x_f, axis=-1, keepdims=True)
        return (x_f * lax.rsqrt(mean_sq + NORM_EPS) * gain).astype(jnp.bfloat16)

    if ffn_layer is not None:
        o_all[mine, :] = o_ref[...]
        pl.semaphore_wait(barrier, len(peers))
        o_x = send(o_ref, o_all.at[mine], sib)
        w_copies = [
            pltpu.make_async_copy(src.at[ffn_layer], dst.at[pl.ds(0, src.shape[1])], w_sem.at[i])
            for i, (src, dst) in enumerate(((wg_hbm, wg), (wu_hbm, wu), (wd_hbm, wd)))
        ]
        hidden, hidden_pad = wu_hbm.shape[1], wu.shape[0]
        for w in (wu, wg, wd):
            w[pl.ds(hidden, hidden_pad - hidden), :] = jnp.zeros((hidden_pad - hidden, d_model), jnp.bfloat16)
        o_x.wait_recv()
        proj_x = []
        for n in range(n_o):
            cols = pl.ds(n * TILE, TILE)
            for k in range(k_steps):
                t = n * k_steps + k
                o_copy(t).wait()
                d = jnp.dot(o_all[:, pl.ds(k * depth, depth)], wt[t], preferred_element_type=jnp.float32)
                if k == 0:
                    proj[:, cols] = d
                else:
                    proj[:, cols] += d
                if t == k_steps - 1:
                    for c in w_copies:
                        c.start()
            proj_x.append(send(proj.at[theirs, cols], proj_in.at[:, cols], sib))
        mine_cols = pl.ds(pl.multiple_of(core * (d_model // 2), d_model // 2), d_model // 2)
        their_cols = pl.ds(pl.multiple_of(other * (d_model // 2), d_model // 2), d_model // 2)
        x_mid[:, mine_cols] = (x_ref[:, mine_cols].astype(jnp.float32) + proj[mine, :]).astype(jnp.bfloat16)
        for c in proj_x:
            c.wait_recv()
        x_mid[:, their_cols] = (x_ref[:, their_cols].astype(jnp.float32) + proj_in[...]).astype(jnp.bfloat16)
        if q_layer is not None:
            for t in range(n_q):
                q_copy(t).start()

        def at(block, c, sub, n):
            return pl.ds(block * 2 * rows + c * rows + sub * half, n)

        g_all[at(OWN, core, 0, rows), :] = norm(x_mid[...].astype(jnp.float32), fgain_ref[ffn_layer:ffn_layer + 1, :])
        a_rows, b_rows = at(OWN, core, 0, half), at(OWN, core, 1, half)
        ag_la = send(g_all.at[a_rows], g_all.at[at(NEAR, core, 1, half)], right)
        ag_rb = send(g_all.at[b_rows], g_all.at[at(NEAR, core, 0, half)], left)
        ag_lb = send(g_all.at[b_rows], g_all.at[at(NEXT, core, 1, half)], right)
        ag_ra = send(g_all.at[a_rows], g_all.at[at(NEXT, core, 0, half)], left)

        def share(block):
            r = at(block, core, 0, rows)
            return send(g_all.at[r], g_all.at[r], sib)

        own_x = share(OWN)

        def gate_up(block, j0=0, j1=hidden_pad // HID_TILE):
            lo = block * 2 * rows

            def body(j, carry):
                cols = pl.ds(pl.multiple_of(j * HID_TILE, HID_TILE), HID_TILE)
                g = g_all[pl.ds(lo, 2 * rows), :]
                gate = lax.dot_general(g, wg[cols, :], NT, preferred_element_type=jnp.float32)
                up = lax.dot_general(g, wu[cols, :], NT, preferred_element_type=jnp.float32)
                act[:, cols] = (jax.nn.silu(gate) * up).astype(jnp.bfloat16)
                return carry

            lax.fori_loop(j0, j1, body, 0)

        def down(block):
            lo = block * 2 * rows

            def body(j, carry):
                cols = pl.ds(pl.multiple_of(j * HID_TILE, HID_TILE), HID_TILE)
                part[pl.ds(lo, 2 * rows), cols] = jnp.dot(
                    act[...], wd[:, cols], preferred_element_type=jnp.float32)
                return carry

            lax.fori_loop(0, d_model // HID_TILE, body, 0)

        def to_sib(block):
            return send(part.at[at(block, other, 0, rows)], sib_in.at[block], sib)

        def add_sib(block):
            r = at(block, core, 0, rows)
            part[r, :] = part[r, :] + sib_in[block]

        ag_la.wait_recv()
        fwd_r = send(g_all.at[at(NEAR, core, 1, half)], g_all.at[at(FAR, core, 0, half)], right)
        ag_rb.wait_recv()
        fwd_l = send(g_all.at[at(NEAR, core, 0, half)], g_all.at[at(FAR, core, 1, half)], left)
        near_x = share(NEAR)
        for c in w_copies:
            c.wait()
        near_x.wait_recv()
        gate_up(NEAR)
        down(NEAR)
        rs_near = to_sib(NEAR)

        ag_lb.wait_recv()
        ag_ra.wait_recv()
        next_x = share(NEXT)
        fwd_r.wait_recv()
        fwd_l.wait_recv()
        far_x = share(FAR)

        rs_near.wait_recv()
        add_sib(NEAR)
        direct_r = send(part.at[at(NEAR, core, 0, half)], fin_l.at[pl.ds(half, half)], right)
        direct_l = send(part.at[at(NEAR, core, 1, half)], fin_r.at[pl.ds(0, half)], left)

        far_x.wait_recv()
        gate_up(FAR)
        down(FAR)
        rs_far = to_sib(FAR)
        next_x.wait_recv()
        gate_up(NEXT, 0, 1)
        rs_far.wait_recv()
        add_sib(FAR)
        opp = []
        for i in range(2):
            q = pl.ds(i * quarter, quarter)
            lo = FAR * 2 * rows + core * rows + i * quarter
            opp.append((send(part.at[pl.ds(lo, quarter)], mid_l.at[q], right),
                        send(part.at[pl.ds(lo + half, quarter)], mid_r.at[q], left)))
        gate_up(NEXT, 1)
        down(NEXT)
        rs_next = to_sib(NEXT)
        own_x.wait_recv()
        gate_up(OWN, 0, 1)
        rs_next.wait_recv()
        add_sib(NEXT)
        merged = []
        for i in range(2):
            q = pl.ds(i * quarter, quarter)
            lo = NEXT * 2 * rows + core * rows + i * quarter
            opp[i][0].wait_recv()
            r = pl.ds(lo, quarter)
            part[r, :] = part[r, :] + mid_l[q, :]
            merged.append(send(part.at[r], fin_l.at[q], right))
            opp[i][1].wait_recv()
            r = pl.ds(lo + half, quarter)
            part[r, :] = part[r, :] + mid_r[q, :]
            merged.append(send(part.at[r], fin_r.at[pl.ds(half + i * quarter, quarter)], left))
        gate_up(OWN, 1)
        down(OWN)
        rs_own = to_sib(OWN)
        rs_own.wait_recv()
        add_sib(OWN)
        for c in (direct_r, direct_l, *merged):
            c.wait_recv()
        total = part[at(OWN, core, 0, rows), :] + fin_l[...] + fin_r[...]
        xout_ref[...] = (x_mid[...].astype(jnp.float32) + total).astype(jnp.bfloat16)
        x_new = xout_ref
    else:
        pl.semaphore_wait(barrier, len(peers))
        x_new = x_ref

    if q_layer is not None:
        h_all[mine, :] = norm(x_new[...].astype(jnp.float32), again_ref[q_layer:q_layer + 1, :])
        h_x = send(h_all.at[mine], h_all.at[mine], sib)
        h_x.wait_recv()
        group = 3
        q_x = []
        for t0 in range(0, n_q, group):
            for t in range(t0, t0 + group):
                q_copy(t).wait()
                q_all[:, pl.ds(t * TILE, TILE)] = jnp.dot(
                    h_all[...], wt[t], preferred_element_type=jnp.float32).astype(jnp.bfloat16)
            cols = pl.ds(t0 * TILE, group * TILE)
            q_x.append(send(q_all.at[theirs, cols], q_in.at[:, cols], sib))
        q_cols = q_ref.shape[1] // 2
        q_ref[:, pl.ds(pl.multiple_of(core * q_cols, q_cols), q_cols)] = q_all[mine, :]
        for c in q_x:
            c.wait_recv()
        q_ref[:, pl.ds(pl.multiple_of(other * q_cols, q_cols), q_cols)] = q_in[...]
    for c in copies:
        c.wait_send()


def dense(ffn_layer, q_layer, n_dp, x_rows, o, fgain, again, wo, wu_t, wg_t, wd, wq):
    rows, d_model = x_rows.shape
    hidden = wd.shape[1]
    hidden_pad = pl.cdiv(hidden, HID_TILE) * HID_TILE
    all_rows = rows * n_dp
    q_cols = wq.shape[2]
    vmem = pl.BlockSpec(memory_space=pltpu.VMEM)
    hbm = pl.BlockSpec(memory_space=pl.ANY)
    bf16, f32 = jnp.bfloat16, jnp.float32
    n_tiles = max(q_cols // 2 // TILE, wo.shape[1] // d_model * (d_model // 2 // TILE))
    args, in_specs, outs = [x_rows], [vmem], []
    scratch = [pltpu.VMEM((n_tiles, d_model, TILE), bf16)]
    if ffn_layer is not None:
        args += [o, fgain, wo, wu_t, wg_t, wd]
        in_specs += [vmem, vmem, hbm, hbm, hbm, hbm]
        outs.append(jax.ShapeDtypeStruct((rows, d_model), bf16))
        scratch += [
            pltpu.VMEM((2 * rows, o.shape[1]), bf16),
            pltpu.VMEM((2 * rows, d_model // 2), f32),
            pltpu.VMEM((rows, d_model // 2), f32),
            pltpu.VMEM((rows, d_model), bf16),
            pltpu.VMEM((hidden_pad, d_model), bf16),
            pltpu.VMEM((hidden_pad, d_model), bf16),
            pltpu.VMEM((hidden_pad, d_model), bf16),
            pltpu.VMEM((all_rows, d_model), bf16),
            pltpu.VMEM((2 * rows, hidden_pad), bf16),
            pltpu.VMEM((all_rows, d_model), f32),
            pltpu.VMEM((4, rows, d_model), f32),
            pltpu.VMEM((rows // 2, d_model), f32),
            pltpu.VMEM((rows // 2, d_model), f32),
            pltpu.VMEM((rows, d_model), f32),
            pltpu.VMEM((rows, d_model), f32),
        ]
    if q_layer is not None:
        args += [again, wq]
        in_specs += [vmem, hbm]
        outs.append(jax.ShapeDtypeStruct((rows, q_cols), bf16))
        scratch += [
            pltpu.VMEM((2 * rows, d_model), bf16),
            pltpu.VMEM((2 * rows, q_cols // 2), bf16),
            pltpu.VMEM((rows, q_cols // 2), bf16),
        ]
    scratch += [
        pltpu.SemaphoreType.DMA((n_tiles,)),
        pltpu.SemaphoreType.DMA((3,)),
        pltpu.SemaphoreType.DMA((N_COPIES,)),
        pltpu.SemaphoreType.DMA((N_COPIES,)),
    ]
    return pl.pallas_call(
        functools.partial(dense_kernel, ffn_layer, q_layer, n_dp),
        out_shape=outs,
        in_specs=in_specs,
        out_specs=[vmem] * len(outs),
        scratch_shapes=scratch,
        compiler_params=pltpu.CompilerParams(
            collective_id=0 if ffn_layer is None else ffn_layer + 1, has_side_effects=True,
            vmem_limit_bytes=(24 if ffn_layer is None else 60) * 2**20),
        name=f"dense_{ffn_layer}_{q_layer}",
    )(*args)


def solution(mesh):
    row_axes = ('replica', 'dp')
    n_dp = mesh.shape['dp']

    def local_step(x_rows, lengths, cache, attn_gain, ffn_gain, w_query, w_attn_out, w_up, w_gate, w_down):
        cache_t = jnp.swapaxes(cache, 2, 3)
        wu_t = jnp.swapaxes(w_up, 1, 2)
        wg_t = jnp.swapaxes(w_gate, 1, 2)
        layers, rows, seq, kv_dim = cache.shape
        heads = w_query.shape[2] // kv_dim
        latent = w_attn_out.shape[1] // heads
        weights = (ffn_gain, attn_gain, w_attn_out, wu_t, wg_t, w_down, w_query)
        (q,) = dense(None, 0, n_dp, x_rows, None, *weights)
        for l in range(layers):
            o = attention(l, latent, q.reshape(rows, heads, kv_dim), cache_t, lengths)
            o = o.reshape(rows, heads * latent)
            if l + 1 < layers:
                x_rows, q = dense(l, l + 1, n_dp, x_rows, o, *weights)
            else:
                (x_rows,) = dense(l, None, n_dp, x_rows, o, *weights)
        return x_rows

    return jax.shard_map(
        local_step,
        mesh=mesh,
        in_specs=(P(row_axes, None), P(row_axes), P(None, row_axes, None, None), P(), P(), P(), P(),
                  P(None, None, 'dp'), P(None, None, 'dp'), P(None, 'dp', None)),
        out_specs=P(row_axes, None),
        check_vma=False,
    )
```

```python
import functools

import jax
import jax.numpy as jnp
from jax import lax
from jax.experimental import pallas as pl
from jax.experimental.pallas import tpu as pltpu
from jax.sharding import PartitionSpec as P

NORM_EPS = 1e-6
MESH = pl.DeviceIdType.MESH
NT = (((1,), (1,)), ((), ()))
GROUP = 8
DEPTH = 3
TILE = 512
HID_TILE = 512
DOWN_TILE = 1024
COPIES = 31

NEAR, FAR, NEXT, OWN = 0, 1, 2, 3


def norm(x_f, gain):
    mean_sq = jnp.mean(x_f * x_f, axis=-1, keepdims=True)
    return (x_f * lax.rsqrt(mean_sq + NORM_EPS) * gain).astype(jnp.bfloat16)


def kernel(n_dp, latent,
           x_hbm, len_ref, cache, again_hbm, fgain_hbm, wq_hbm, wo_hbm, wu_hbm, wg_hbm, wd_hbm,
           out_ref,
           x_cur, again, fgain, wt, h_all, q_all, q_in, q_heads, o_heads, o_all, proj, proj_in,
           g_all, part, sib_in, mid_l, mid_r, fin_l, fin_r,
           in_sem, wt_sem, send_sem, recv_sem):
    me = lax.axis_index("dp")
    chips = n_dp // 2
    chip, core = me // 2, lax.rem(me, 2)
    other = 1 - core
    sib = chip * 2 + other
    right = lax.rem(chip + 1, chips) * 2 + core
    left = lax.rem(chip + chips - 1, chips) * 2 + core
    peers = (sib, left, right)
    layers, rows, kv, seq = cache.shape
    d_model = x_cur.shape[1]
    half, quarter = rows // 2, rows // 4
    q_cols = q_all.shape[1]
    heads = 2 * q_cols // kv
    scale = (3 * (kv - latent)) ** -0.5
    depth = wt.shape[1]
    n_q = q_cols // TILE
    k_steps = o_all.shape[1] // depth
    n_o = d_model // 2 // TILE
    hidden, hidden_pad = wu_hbm.shape[1], pl.cdiv(wu_hbm.shape[1], 128) * 128
    groups = rows // GROUP
    mine, theirs = pl.ds(core * rows, rows), pl.ds(other * rows, rows)

    def q_copy(l, t):
        lo = pl.multiple_of(core * q_cols + t * TILE, 128)
        return pltpu.make_async_copy(wq_hbm.at[l, :, pl.ds(lo, TILE)], wt.at[t], wt_sem.at[t])

    def o_copy(l, t):
        n, k = t // k_steps, lax.rem(t, k_steps)
        lo = pl.multiple_of(core * (d_model // 2) + n * TILE, TILE)
        return pltpu.make_async_copy(
            wo_hbm.at[l, pl.ds(pl.multiple_of(k * depth, depth), depth), pl.ds(lo, TILE)],
            wt.at[t], wt_sem.at[t])

    copies = []
    left_over = []

    def sent(*done):
        for c in done:
            c.wait_send()
        left_over[:] = [c for c in left_over if all(c is not d for d in done)]

    def send(src, dst, peer):
        k = len(copies)
        c = pltpu.make_async_remote_copy(
            src_ref=src, dst_ref=dst, send_sem=send_sem.at[k], recv_sem=recv_sem.at[k],
            device_id={"dp": peer}, device_id_type=MESH)
        copies.append(c)
        left_over.append(c)
        c.start()
        return c

    barrier = pltpu.get_barrier_semaphore()
    for peer in peers:
        pl.semaphore_signal(barrier, inc=1, device_id={"dp": peer}, device_id_type=MESH)
    first = [pltpu.make_async_copy(src, dst, in_sem.at[i])
             for i, (src, dst) in enumerate(((x_hbm, x_cur), (again_hbm, again), (fgain_hbm, fgain)))]
    for c in first:
        c.start()
    for t in range(n_q):
        q_copy(0, t).start()
    for c in first:
        c.wait()

    def attention(l, buf, sem):
        def start(g):
            for i in range(GROUP):
                pltpu.make_async_copy(
                    cache.at[l, g * GROUP + i], buf.at[lax.rem(g, DEPTH), i], sem.at[lax.rem(g, DEPTH)]).start()

        h_all[mine, :] = norm(x_cur[...].astype(jnp.float32), again[l:l + 1, :])
        if l == 0:
            pl.semaphore_wait(barrier, len(peers))
        h_x = send(h_all.at[mine], h_all.at[mine], sib)
        h_x.wait_recv()
        q_x = []
        step = 3
        for t0 in range(0, n_q, step):
            for t in range(t0, t0 + step):
                q_copy(l, t).wait()
                q_all[:, pl.ds(t * TILE, TILE)] = jnp.dot(
                    h_all[...], wt[t], preferred_element_type=jnp.float32).astype(jnp.bfloat16)
            if t0 == 0:
                for g in range(DEPTH):
                    start(g)
            cols = pl.ds(t0 * TILE, step * TILE)
            q_x.append(send(q_all.at[theirs, cols], q_in.at[:, cols], sib))

        lanes = [(c, min(128, kv - c)) for c in range(0, kv, 128)]

        def query_of(b):
            parts = [q_heads[n, pl.ds(b, heads, stride=rows), :] for n in range(len(lanes))]
            return jnp.concatenate(parts, axis=1)[:, :kv].astype(jnp.bfloat16)

        def split(src, src_rows, first_head):
            for j in range(0, heads // 2, 2):
                pair = src[src_rows, pl.ds(j * kv, 2 * kv)].astype(jnp.float32)
                for i in range(2):
                    lo = pl.multiple_of((first_head + j + i) * rows, rows)
                    for n, (c, w) in enumerate(lanes):
                        q_heads[n, pl.ds(lo, rows), pl.ds(0, w)] = pair[:, i * kv + c:i * kv + c + w]

        split(q_all, mine, core * (heads // 2))
        for c in q_x:
            c.wait_recv()
        split(q_in, pl.ds(0, rows), other * (heads // 2))

        def body(g, carry):
            slot = lax.rem(g, DEPTH)
            o_copy(l, g).start()
            pltpu.make_async_copy(cache.at[l, pl.ds(g * GROUP, GROUP)], buf.at[slot], sem.at[slot]).wait()
            bs = [g * GROUP + i for i in range(GROUP)]
            s = [jnp.dot(query_of(b), buf[slot, i], preferred_element_type=jnp.float32) for i, b in enumerate(bs)]
            pos = lax.broadcasted_iota(jnp.int32, (heads, seq), 1)
            s = [jnp.where(pos < len_ref[b], x * scale, -jnp.inf) for x, b in zip(s, bs)]
            e = [jnp.exp(x - jnp.max(x, axis=1, keepdims=True)) for x in s]
            p = [(x / jnp.sum(x, axis=1, keepdims=True)).astype(jnp.bfloat16) for x in e]
            o = [lax.dot_general(x, buf[slot, i, pl.ds(0, latent), :], NT, preferred_element_type=jnp.float32)
                 for i, x in enumerate(p)]
            for x, b in zip(o, bs):
                for n in range(latent // 128):
                    o_heads[n, pl.ds(b, heads, stride=rows), :] = x[:, n * 128:(n + 1) * 128]

            @pl.when(g + DEPTH < groups)
            def _():
                start(g + DEPTH)

            return carry

        lax.fori_loop(0, groups, body, 0)
        sent(h_x, *q_x)

    def feed_forward(l, wg, wu, wd, act, st0, st1, st2, w_sem):
        stages = (st0, st1, st2)
        tiles = [(lo, min(HID_TILE, hidden_pad - lo)) for lo in range(0, hidden_pad, HID_TILE)]

        def stage_copy(i, c):
            lo, _ = tiles[c]
            n = min(HID_TILE, hidden - lo)
            return pltpu.make_async_copy(
                (wg_hbm, wu_hbm)[i].at[l, pl.ds(lo, n)], stages[c].at[pl.ds(0, n)], w_sem.at[c])

        def transpose(i, c):
            lo, n = tiles[c]
            dst = (wg, wu)[i]

            def body(j, carry):
                r = pl.ds(pl.multiple_of(j * TILE, TILE), TILE)
                dst[r, pl.ds(lo, n)] = stages[c][:, r].T
                return carry

            lax.fori_loop(0, d_model // TILE, body, 0)

        for c in range(len(tiles)):
            stage_copy(0, c).start()
        wd_copy = pltpu.make_async_copy(wd_hbm.at[l], wd.at[pl.ds(0, hidden)], w_sem.at[len(tiles)])
        wd_copy.start()
        pad = jnp.zeros((hidden_pad - hidden, d_model), jnp.bfloat16)
        wd[pl.ds(hidden, hidden_pad - hidden), :] = pad
        last = hidden - tiles[-1][0]
        st2[pl.ds(last, hidden_pad - hidden), :] = pad

        for h in range(heads):
            for n in range(latent // 128):
                o_all[mine, pl.ds(h * latent + n * 128, 128)] = o_heads[n, pl.ds(h * rows, rows), :].astype(jnp.bfloat16)
        o_x = send(o_all.at[mine], o_all.at[mine], sib)
        o_x.wait_recv()
        proj_x = []
        for n in range(n_o):
            cols = pl.ds(n * TILE, TILE)
            for k in range(k_steps):
                t = n * k_steps + k
                o_copy(l, t).wait()
                d = jnp.dot(o_all[:, pl.ds(k * depth, depth)], wt[t], preferred_element_type=jnp.float32)
                if k == 0:
                    proj[:, cols] = d
                else:
                    proj[:, cols] += d
            proj_x.append(send(proj.at[theirs, cols], proj_in.at[:, cols], sib))
        mine_cols = pl.ds(pl.multiple_of(core * (d_model // 2), d_model // 2), d_model // 2)
        their_cols = pl.ds(pl.multiple_of(other * (d_model // 2), d_model // 2), d_model // 2)
        x_cur[:, mine_cols] = (x_cur[:, mine_cols].astype(jnp.float32) + proj[mine, :]).astype(jnp.bfloat16)
        for c in proj_x:
            c.wait_recv()
        x_cur[:, their_cols] = (x_cur[:, their_cols].astype(jnp.float32) + proj_in[...]).astype(jnp.bfloat16)

        def at(block, c, sub, n):
            return pl.ds(block * 2 * rows + c * rows + sub * half, n)

        g_all[at(OWN, core, 0, rows), :] = norm(x_cur[...].astype(jnp.float32), fgain[l:l + 1, :])
        a_rows, b_rows = at(OWN, core, 0, half), at(OWN, core, 1, half)
        ag_la = send(g_all.at[a_rows], g_all.at[at(NEAR, core, 1, half)], right)
        ag_rb = send(g_all.at[b_rows], g_all.at[at(NEAR, core, 0, half)], left)
        ag_lb = send(g_all.at[b_rows], g_all.at[at(NEXT, core, 1, half)], right)
        ag_ra = send(g_all.at[a_rows], g_all.at[at(NEXT, core, 0, half)], left)

        def share(block):
            r = at(block, core, 0, rows)
            return send(g_all.at[r], g_all.at[r], sib)

        own_x = share(OWN)

        for c in range(len(tiles)):
            stage_copy(0, c).wait()
            transpose(0, c)
            stage_copy(1, c).start()
        ag_la.wait_recv()
        fwd_r = send(g_all.at[at(NEAR, core, 1, half)], g_all.at[at(FAR, core, 0, half)], right)
        ag_rb.wait_recv()
        fwd_l = send(g_all.at[at(NEAR, core, 0, half)], g_all.at[at(FAR, core, 1, half)], left)
        near_x = share(NEAR)
        for c in range(len(tiles)):
            stage_copy(1, c).wait()
            transpose(1, c)
        wd_copy.wait()
        if l + 1 < layers:
            for t in range(n_q):
                q_copy(l + 1, t).start()

        def gate_up(block, j0=0, j1=len(tiles)):
            for lo, n in tiles[j0:j1]:
                cols = pl.ds(lo, n)
                g = g_all[pl.ds(block * 2 * rows, 2 * rows), :]
                gate = jnp.dot(g, wg[:, cols], preferred_element_type=jnp.float32)
                up = jnp.dot(g, wu[:, cols], preferred_element_type=jnp.float32)
                act[:, cols] = (jax.nn.silu(gate) * up).astype(jnp.bfloat16)

        def down(block):
            for lo in range(0, d_model, DOWN_TILE):
                cols = pl.ds(lo, DOWN_TILE)
                part[pl.ds(block * 2 * rows, 2 * rows), cols] = jnp.dot(
                    act[...], wd[:, cols], preferred_element_type=jnp.float32)

        def to_sib(block):
            return send(part.at[at(block, other, 0, rows)], sib_in.at[block], sib)

        def add_sib(block):
            r = at(block, core, 0, rows)
            part[r, :] = part[r, :] + sib_in[block]

        near_x.wait_recv()
        gate_up(NEAR)
        down(NEAR)
        rs_near = to_sib(NEAR)

        ag_lb.wait_recv()
        ag_ra.wait_recv()
        next_x = share(NEXT)
        fwd_r.wait_recv()
        fwd_l.wait_recv()
        far_x = share(FAR)

        rs_near.wait_recv()
        add_sib(NEAR)
        sent(fwd_r, fwd_l, near_x)
        direct_r = send(part.at[at(NEAR, core, 0, half)], fin_l.at[pl.ds(half, half)], right)
        direct_l = send(part.at[at(NEAR, core, 1, half)], fin_r.at[pl.ds(0, half)], left)

        far_x.wait_recv()
        gate_up(FAR)
        down(FAR)
        rs_far = to_sib(FAR)
        next_x.wait_recv()
        gate_up(NEXT, 0, 2)
        rs_far.wait_recv()
        add_sib(FAR)
        sent(far_x, next_x)
        opp = []
        for i in range(2):
            q = pl.ds(i * quarter, quarter)
            lo = FAR * 2 * rows + core * rows + i * quarter
            opp.append((send(part.at[pl.ds(lo, quarter)], mid_l.at[q], right),
                        send(part.at[pl.ds(lo + half, quarter)], mid_r.at[q], left)))
        gate_up(NEXT, 2)
        down(NEXT)
        rs_next = to_sib(NEXT)
        own_x.wait_recv()
        gate_up(OWN, 0, 2)
        rs_next.wait_recv()
        add_sib(NEXT)
        gate_up(OWN, 2)
        down(OWN)
        rs_own = to_sib(OWN)
        merged = []
        for i in range(2):
            q = pl.ds(i * quarter, quarter)
            lo = NEXT * 2 * rows + core * rows + i * quarter
            opp[i][0].wait_recv()
            r = pl.ds(lo, quarter)
            part[r, :] = part[r, :] + mid_l[q, :]
            merged.append(send(part.at[r], fin_l.at[q], right))
            opp[i][1].wait_recv()
            r = pl.ds(lo + half, quarter)
            part[r, :] = part[r, :] + mid_r[q, :]
            merged.append(send(part.at[r], fin_r.at[pl.ds(half + i * quarter, quarter)], left))
        rs_own.wait_recv()
        add_sib(OWN)
        for c in (direct_r, direct_l, *merged):
            c.wait_recv()
        total = part[at(OWN, core, 0, rows), :] + fin_l[...] + fin_r[...]
        x_cur[...] = (x_cur[...].astype(jnp.float32) + total).astype(jnp.bfloat16)
        sent(*list(left_over))

    bf16 = jnp.bfloat16
    for l in range(layers):
        pl.run_scoped(
            functools.partial(attention, l),
            pltpu.VMEM((DEPTH, GROUP, kv, seq), bf16),
            pltpu.SemaphoreType.DMA((DEPTH,)))
        pl.run_scoped(
            functools.partial(feed_forward, l),
            pltpu.VMEM((d_model, hidden_pad), bf16),
            pltpu.VMEM((d_model, hidden_pad), bf16),
            pltpu.VMEM((hidden_pad, d_model), bf16),
            pltpu.VMEM((2 * rows, hidden_pad), bf16),
            pltpu.VMEM((HID_TILE, d_model), bf16),
            pltpu.VMEM((HID_TILE, d_model), bf16),
            pltpu.VMEM((hidden_pad - 2 * HID_TILE, d_model), bf16),
            pltpu.SemaphoreType.DMA((4,)))
    out_ref[...] = x_cur[...]


def solution(mesh):
    row_axes = ('replica', 'dp')
    n_dp = mesh.shape['dp']

    def local_step(x_rows, lengths, cache, attn_gain, ffn_gain, w_query, w_attn_out, w_up, w_gate, w_down):
        layers, rows, seq, kv = cache.shape
        d_model = x_rows.shape[1]
        heads = w_query.shape[2] // kv
        latent = w_attn_out.shape[1] // heads
        q_cols = w_query.shape[2] // 2
        all_rows = rows * n_dp
        bf16, f32 = jnp.bfloat16, jnp.float32
        vmem = pl.BlockSpec(memory_space=pltpu.VMEM)
        hbm = pl.BlockSpec(memory_space=pl.ANY)
        n_tiles = max(q_cols // TILE, w_attn_out.shape[1] // d_model * (d_model // 2 // TILE))
        return pl.pallas_call(
            functools.partial(kernel, n_dp, latent),
            out_shape=jax.ShapeDtypeStruct((rows, d_model), bf16),
            in_specs=[hbm, pl.BlockSpec(memory_space=pltpu.SMEM)] + [hbm] * 8,
            out_specs=vmem,
            scratch_shapes=[
                pltpu.VMEM((rows, d_model), bf16),
                pltpu.VMEM(attn_gain.shape, f32),
                pltpu.VMEM(ffn_gain.shape, f32),
                pltpu.VMEM((n_tiles, d_model, TILE), bf16),
                pltpu.VMEM((2 * rows, d_model), bf16),
                pltpu.VMEM((2 * rows, q_cols), bf16),
                pltpu.VMEM((rows, q_cols), bf16),
                pltpu.VMEM((pl.cdiv(kv, 128), heads * rows, 128), f32),
                pltpu.VMEM((latent // 128, heads * rows, 128), f32),
                pltpu.VMEM((2 * rows, heads * latent), bf16),
                pltpu.VMEM((2 * rows, d_model // 2), f32),
                pltpu.VMEM((rows, d_model // 2), f32),
                pltpu.VMEM((all_rows, d_model), bf16),
                pltpu.VMEM((all_rows, d_model), f32),
                pltpu.VMEM((4, rows, d_model), f32),
                pltpu.VMEM((rows // 2, d_model), f32),
                pltpu.VMEM((rows // 2, d_model), f32),
                pltpu.VMEM((rows, d_model), f32),
                pltpu.VMEM((rows, d_model), f32),
                pltpu.SemaphoreType.DMA((3,)),
                pltpu.SemaphoreType.DMA((n_tiles,)),
                pltpu.SemaphoreType.DMA((layers * COPIES,)),
                pltpu.SemaphoreType.DMA((layers * COPIES,)),
            ],
            compiler_params=pltpu.CompilerParams(
                collective_id=0, has_side_effects=True, vmem_limit_bytes=67_043_328),
            name="decode_layers",
        )(x_rows, lengths, jnp.swapaxes(cache, 2, 3), attn_gain, ffn_gain, w_query, w_attn_out,
          jnp.swapaxes(w_up, 1, 2), jnp.swapaxes(w_gate, 1, 2), w_down)

    return jax.shard_map(
        local_step,
        mesh=mesh,
        in_specs=(P(row_axes, None), P(row_axes), P(None, row_axes, None, None), P(), P(), P(), P(),
                  P(None, None, 'dp'), P(None, None, 'dp'), P(None, 'dp', None)),
        out_specs=P(row_axes, None),
        check_vma=False,
    )
```
